256 devices in a mesh: dof: 16 (over x, y_hi, core), tm: 16 (over z, y_lo).
Axes of the slice: x: 4, y: 4 (y_hi: 2, y_lo: 2; y = y_hi * 2 + y_lo), z: 8, core: 2. Of those that a mesh axis runs over, the one named last changes fastest.
Arguments:
- snapshots: bfloat16 [327680, 4096], P('dof', 'tm'), may hold values from -6 to 6
- basis: bfloat16 [327680, 64], P('dof'), may hold values from -0.009765625 to 0.009765625
Outputs:
- gram: float32 [2144, 2144], P('tm', 'dof')
- coords: float32 [64, 4096], P(None, 'tm')
The draws below stay inside these ranges and needn't reach their ends.
All inputs are finite; a program needn't handle non-finite values.
Results may differ from the reference program's by a relative error of at most 0.0021.
Values may be sent and summed in bfloat16 or wider, within the bound.
A program may use at most 64 MiB of HBM per device.

```python
import jax
import jax.numpy as jnp
import numpy as np
from jax import lax

R = 64
NDOF = 327680
NT = 4096


def level_of(rng, shape, cuts, least, high):
    factor_of = 1.0
    for axis_at, parts in cuts:
        draws = jax.random.uniform(jax.random.fold_in(jax.random.fold_in(rng, 6), axis_at), (parts,), jnp.float32, least / len(cuts), high / len(cuts))
        factor_of = factor_of * jnp.repeat(jnp.exp(draws), shape[axis_at] // parts).reshape((-1,) + (1,) * (len(shape) - 1 - axis_at))
    return factor_of


def gaussian(key, shape, deviation, reach, pieces=(), held_as=jnp.bfloat16):
    result = jax.random.normal(key, shape, jnp.float32) * deviation
    if len(pieces) > 0:
        result = level_of(key, shape, pieces, -0.22, 0.18) * result
    return jnp.clip(result, min=-reach, max=reach).astype(held_as)


def setup_inputs(seed: int = 0) -> dict:
    keys = jax.random.split(jax.random.key(seed), 3)
    return {
        "snapshots": gaussian(keys[0], (NDOF, NT), 1.0, 6.0, ((0, 16), (1, 16))),
        "basis": gaussian(keys[1], (NDOF, R), NDOF ** -0.5, 0.009765625, ((0, 16),)),
    }


def build_features(coords):
    modes = coords.shape[0]
    upper_i, upper_j = np.triu_indices(modes)
    quad = coords[upper_i, :] * coords[upper_j, :]
    return jnp.concatenate([coords, quad], axis=0).astype(jnp.bfloat16)


def reference(snapshots, basis):
    coords = lax.dot_general(basis, snapshots, (((0,), (0,)), ((), ())), preferred_element_type=jnp.float32)
    features = build_features(coords)
    gram = lax.dot_general(features, features, (((1,), (1,)), ((), ())), preferred_element_type=jnp.float32)
    gram = gram * (1.0 / NT)
    return gram, coords
```

```python
import functools

import jax
import jax.numpy as jnp
from jax import lax
from jax.experimental import pallas as pl
from jax.experimental.pallas import tpu as pltpu
from jax.sharding import PartitionSpec as P

MESH = pl.DeviceIdType.MESH
R = 64
NT = 4096
W = 134
PAD = 144
CHUNKS = 20


def one_hot_pair(block):
    shape = (PAD, 256)
    feature = block * W + lax.broadcasted_iota(jnp.int32, shape, 0)
    lane = lax.broadcasted_iota(jnp.int32, shape, 1)
    mode = lane & (R - 1)
    data = lane < 3 * R
    pair = feature - R
    linear = feature < R
    start = mode * R - ((mode * (mode - 1)) >> 1)
    first = (start <= pair) & (pair < start + R - mode)
    shift = jnp.where(first & (lane < R), (mode - start).astype(jnp.float32), 0.0)
    second = pair.astype(jnp.float32) + jnp.sum(shift, axis=1, keepdims=True)
    def num(mask):
        return jnp.where(mask, jnp.float32(1), jnp.float32(0))

    hot_i = jnp.where(linear, num(mode == feature), num(first)) * num(data)
    hot_j = jnp.where(
        linear, num(lane == 3 * R), num(mode.astype(jnp.float32) == second) * num(data)
    )
    return hot_i.astype(jnp.bfloat16), hot_j.astype(jnp.bfloat16)


def kernel(
    basis_hbm, snap_hbm, gram_ref, coords_ref,
    basis, snap, hot_i, hot_j, part, got, tiles, gram_acc, gram_in, other_half,
    load_sem, rs_send, rs_recv, z_send, z_recv, p_send, p_recv, c_send, c_recv, g_send, g_recv,
):
    d = lax.axis_index("dof")
    t = lax.axis_index("tm")
    core = lax.rem(d, 2)
    group = d // 2
    x = d // 4
    y_hi = lax.rem(group, 2)
    z = t // 2
    y_lo = lax.rem(t, 2)
    chip = x * 4 + y_hi * 2 + y_lo
    partner = d + 1 - 2 * core
    depth = basis.shape[1] // CHUNKS

    def load(i):
        at = pl.ds(pl.multiple_of(i * depth, depth), depth)
        return (
            pltpu.make_async_copy(basis_hbm.at[:, at], basis.at[:, at], load_sem.at[0, i]),
            pltpu.make_async_copy(snap_hbm.at[at], snap.at[at], load_sem.at[1, i]),
        )

    def start_load(i, _):
        for copy in load(i):
            copy.start()
        return 0

    lax.fori_loop(0, CHUNKS, start_load, 0)

    barrier = pltpu.get_barrier_semaphore()

    def greet_dof(k, _):
        pl.semaphore_signal(
            barrier, inc=1, device_id={"dof": lax.rem(d + k, 16), "tm": t}, device_id_type=MESH
        )
        return 0

    def greet_z(k, _):
        to = lax.rem(z + k, 8) * 2 + y_lo
        pl.semaphore_signal(barrier, inc=1, device_id={"dof": d, "tm": to}, device_id_type=MESH)
        return 0

    def greet_plane(k, _):
        pl.semaphore_signal(
            barrier, inc=1,
            device_id={"dof": k * 2 + core, "tm": z * 2 + 1 - y_lo}, device_id_type=MESH,
        )
        return 0

    lax.fori_loop(1, 16, greet_dof, 0)
    lax.fori_loop(1, 8, greet_z, 0)
    lax.fori_loop(0, 8, greet_plane, 0)

    for n, block in enumerate((t, d, partner)):
        first, second = one_hot_pair(block)
        hot_i[pl.ds(n * PAD, PAD)] = first
        hot_j[pl.ds(n * PAD, PAD)] = second
    gram_acc[...] = jnp.zeros_like(gram_acc)

    def project(i, acc):
        for copy in load(i):
            copy.wait()
        at = pl.ds(pl.multiple_of(i * depth, depth), depth)
        return acc + jnp.dot(basis[:, at], snap[at], preferred_element_type=jnp.float32)

    acc = lax.fori_loop(0, CHUNKS, project, jnp.zeros((R, 256), jnp.float32))
    for g in range(8):
        for h in range(2):
            part[2 * g + h] = acc[8 * g : 8 * g + 8, 128 * h : 128 * h + 128]

    pl.semaphore_wait(barrier, 30)

    def rs_copy(k):
        to = lax.rem(d + k, 16)
        return pltpu.make_async_remote_copy(
            src_ref=part.at[to], dst_ref=got.at[d], send_sem=rs_send, recv_sem=rs_recv,
            device_id={"dof": to, "tm": t}, device_id_type=MESH,
        )

    def rs_start(k, _):
        rs_copy(k).start()
        return 0

    lax.fori_loop(1, 16, rs_start, 0)
    got[d] = part[d]

    def wait_tiles(n, sem):
        fifteen = tiles.at[0, pl.ds(0, n)]
        pltpu.make_async_copy(fifteen, fifteen, sem).wait()

    wait_tiles(15, rs_recv)
    mine = y_lo * 8 + group
    tiles[z, mine] = jnp.sum(got[...], axis=0)

    def z_copy(k):
        to = lax.rem(z + k, 8)
        return pltpu.make_async_remote_copy(
            src_ref=tiles.at[z, mine], dst_ref=tiles.at[z, mine],
            send_sem=z_send.at[to], recv_sem=z_recv.at[z],
            device_id={"dof": d, "tm": to * 2 + y_lo}, device_id_type=MESH,
        )

    def z_start(k, _):
        z_copy(k).start()
        return 0

    lax.fori_loop(1, 8, z_start, 0)

    def order(s):
        return lax.rem(z + 8 + ((s + 1) // 2) * (2 * lax.rem(s, 2) - 1), 8)

    def p_start_at(slot):
        def start(k, _):
            to = lax.rem(chip + k, 16)
            to_x, to_hi, to_lo = to // 4, lax.rem(to // 2, 2), lax.rem(to, 2)
            pltpu.make_async_remote_copy(
                src_ref=tiles.at[slot, mine], dst_ref=tiles.at[slot, mine],
                send_sem=p_send.at[slot], recv_sem=p_recv.at[slot],
                device_id={"dof": (to_x * 2 + to_hi) * 2 + core, "tm": z * 2 + to_lo},
                device_id_type=MESH,
            ).start()
            return 0

        lax.fori_loop(1, 16, start, 0)

    p_start_at(z)

    def forward(s, _):
        slot = order(s)
        here = tiles.at[slot, mine]
        pltpu.make_async_copy(here, here, z_recv.at[slot]).wait()
        p_start_at(slot)
        return 0

    lax.fori_loop(1, 8, forward, 0)

    half = tiles.at[z, pl.ds(y_lo * 8, 8)]
    c_copy = pltpu.make_async_remote_copy(
        src_ref=half, dst_ref=other_half, send_sem=c_send, recv_sem=c_recv,
        device_id={"dof": partner, "tm": t}, device_id_type=MESH,
    )

    def accumulate(slot):
        both = tiles[slot]
        c = jnp.concatenate([both[:8].reshape(R, 128), both[8:].reshape(R, 128)], axis=1)
        hi = c.astype(jnp.bfloat16)
        rest = c - hi.astype(jnp.float32)
        mid = rest.astype(jnp.bfloat16)
        low = (rest - mid.astype(jnp.float32)).astype(jnp.bfloat16)
        table = jnp.concatenate([hi, mid, low, jnp.ones((R, 256), jnp.bfloat16)], axis=0)
        a = jnp.dot(hot_i[...], table, preferred_element_type=jnp.float32)
        b = jnp.dot(hot_j[...], table, preferred_element_type=jnp.float32)
        f = (a * b).astype(jnp.bfloat16)
        rows = f[:PAD]
        for n in range(2):
            gram_acc[n] += lax.dot_general(
                rows, f[(n + 1) * PAD : (n + 2) * PAD], (((1,), (1,)), ((), ())),
                preferred_element_type=jnp.float32,
            )

    wait_tiles(15, p_recv.at[z])
    c_copy.start()
    accumulate(z)

    def step(s, _):
        slot = order(s)
        wait_tiles(15, p_recv.at[slot])
        accumulate(slot)
        return 0

    lax.fori_loop(1, 8, step, 0)

    g_copy = pltpu.make_async_remote_copy(
        src_ref=gram_acc.at[1], dst_ref=gram_in, send_sem=g_send, recv_sem=g_recv,
        device_id={"dof": partner, "tm": t}, device_id_type=MESH,
    )
    g_copy.start()

    wait_tiles(15, rs_send)

    def z_done(k, _):
        z_copy(k).wait_send()
        return 0

    lax.fori_loop(1, 8, z_done, 0)

    def p_done(slot, _):
        wait_tiles(15, p_send.at[slot])
        return 0

    lax.fori_loop(0, 8, p_done, 0)
    c_copy.wait()
    own = tiles[z, pl.ds(y_lo * 8, 8)].reshape(R, 128)
    theirs = other_half[...].reshape(R, 128)
    coords_ref[:, :128] = jnp.where(core == 0, own, theirs)
    coords_ref[:, 128:] = jnp.where(core == 0, theirs, own)
    g_copy.wait()
    total = (gram_acc[0] + gram_in[...]) * (1.0 / NT)
    gram_ref[...] = total[:W, :W]


def on_device(snapshots, basis):
    rows, times = snapshots.shape
    vmem, dma = pltpu.VMEM, pltpu.SemaphoreType.DMA
    return pl.pallas_call(
        kernel,
        out_shape=(
            jax.ShapeDtypeStruct((W, W), jnp.float32),
            jax.ShapeDtypeStruct((R, times), jnp.float32),
        ),
        in_specs=[pl.BlockSpec(memory_space=pltpu.HBM)] * 2,
        out_specs=(pl.BlockSpec(memory_space=vmem), pl.BlockSpec(memory_space=vmem)),
        scratch_shapes=[
            vmem((R, rows), jnp.bfloat16),
            vmem((rows, times), jnp.bfloat16),
            vmem((3 * PAD, 256), jnp.bfloat16),
            vmem((3 * PAD, 256), jnp.bfloat16),
            vmem((16, 8, 128), jnp.float32),
            vmem((16, 8, 128), jnp.float32),
            vmem((8, 16, 8, 128), jnp.float32),
            vmem((2, PAD, PAD), jnp.float32),
            vmem((PAD, PAD), jnp.float32),
            vmem((8, 8, 128), jnp.float32),
            dma((2, CHUNKS)),
            dma, dma, dma((8,)), dma((8,)), dma((8,)), dma((8,)), dma, dma, dma, dma,
        ],
        compiler_params=pltpu.CompilerParams(
            collective_id=0, has_side_effects=True, vmem_limit_bytes=40 << 20
        ),
    )(basis.T, snapshots)


def solution(mesh):
    return jax.shard_map(
        on_device,
        mesh=mesh,
        in_specs=(P("dof", "tm"), P("dof", None)),
        out_specs=(P("tm", "dof"), P(None, "tm")),
        check_vma=False,
    )
```
